256 devices in a mesh: tok: 64 (over z, y, core), voc: 4 (over x).
Axes of the slice: x: 4, y: 4, z: 8, core: 2. Of those that a mesh axis runs over, the one named last changes fastest.
Arguments:
- hidden: bfloat16 [2048, 3584], P(('tok', 'voc')), may hold values from -256 to 256
- norm_gain: float32 [3584], replicated, may hold values from 0.5 to 1.5
- weight: bfloat16 [3584, 152064], P(None, ('tok', 'voc')), may hold values from -5 to 5
- targets: int32 [2048], P(('tok', 'voc')), may hold values from 0 to 152063
- label_mask: int32 [2048], P(('tok', 'voc')), may hold values from 0 to 1, as said below
Outputs:
- token_loss: float32 [2048], P(('tok', 'voc'))
- mean_loss: float32 [], replicated
The draws below stay inside these ranges and needn't reach their ends.
Inputs may be any that keep to these rules, and one draw needn't show every extreme that they name: `label_mask`: position 0 of each of the 2 microbatches of 1024 positions is valid; in each microbatch the valid positions lie before a ragged length of 512 or more.
All inputs are finite; a program needn't handle non-finite values.
Results may differ from the reference program's by a relative error of at most 0.00061.
Values may be sent and summed in bfloat16 or wider, within the bound.
No kernel may reach another device: no remote copies, remote signals or barrier semaphores. Data moves between devices by JAX's collectives and lax.ppermute only.
A program may use at most 128 MiB of HBM per device.

```python
import math
import jax
import jax.numpy as jnp
import numpy as np
from jax import lax

D = 3584
VOC_DEV = 594
VOCAB = 152064
TOKENS = 2048
MICRO = 2
MB_TOK = 1024
N_TOK = 64
N_VOC = 4


def drawn_parts(key):
    planted_key = jax.random.fold_in(key, 901)
    chosen_columns = jax.random.permutation(jax.random.fold_in(planted_key, 1), VOCAB)[:6]
    chosen_rows = jax.random.permutation(jax.random.fold_in(planted_key, 2), TOKENS)[:6]
    sign_bits = jax.random.randint(jax.random.fold_in(planted_key, 3), (3, D), 0, 2)
    directions = 2.0 * sign_bits.astype(jnp.float32) - 1.0
    return (chosen_columns, chosen_rows, directions)


def draw_weight(key, part):
    chosen_columns, chosen_rows, directions = drawn_parts(key)
    rough_part = jax.random.normal(jax.random.fold_in(key, 11), (D, VOCAB), jnp.float32)
    column_scale = jnp.exp(jax.random.uniform(jax.random.fold_in(key, 12), (1, VOCAB), jnp.float32, 0.0, math.log(10.0)))
    matrix = rough_part * column_scale * (0.8 / math.sqrt(D))
    group_of = jnp.array([0, 0, 1, 1, 2, 2], jnp.int32)
    strengths = jnp.array([130.0, 128.0, 195.0, 193.0, 260.0, 257.4], jnp.float32)
    planted = (directions[group_of] * strengths[:, None] / D).T
    matrix = matrix.at[:, chosen_columns].set(planted)
    return jnp.clip(matrix, -5.0, 5.0).astype(jnp.bfloat16)


def draw_hidden(key, part):
    rough_part = jax.random.normal(jax.random.fold_in(key, 22), (TOKENS, D), jnp.float32)
    chosen_columns, chosen_rows, directions = drawn_parts(key)
    group_of = jnp.array([0, 0, 1, 1, 2, 2], jnp.int32)
    row_scale = jnp.exp(jax.random.uniform(jax.random.fold_in(key, 21), (TOKENS, 1), jnp.float32, 0.0, math.log(10.0)))
    states = rough_part * row_scale
    states = states.at[chosen_rows].set(directions[group_of] * 2.0)
    return jnp.clip(states, -256.0, 256.0).astype(jnp.bfloat16)


def draw_label_mask(key, part):
    token_index = jnp.arange(TOKENS, dtype=jnp.int32)
    position = token_index % MB_TOK
    micro_index = token_index // MB_TOK
    lengths = jax.random.randint(jax.random.fold_in(key, 31), (MICRO,), MB_TOK // 2, MB_TOK + 1)
    within = position < lengths[micro_index]
    chance = jax.random.randint(jax.random.fold_in(key, 32), (TOKENS,), 0, 1000)
    kept_token = chance < 250 + 700 * token_index // TOKENS
    valid = jnp.logical_or(jnp.logical_and(within, kept_token), position == 0)
    return valid.astype(jnp.int32)


def set_ends(values, stream_key, low, high):
    dims = values.shape
    place = [jax.random.randint(jax.random.fold_in(stream_key, axis), (), 0, dims[axis]) for axis in range(len(dims))]
    values = values.at[tuple(place)].set(low)
    longest = dims.index(max(dims))
    place[longest] = (place[longest] + 1) % dims[longest]
    return values.at[tuple(place)].set(high)


def wide_ids(own_key, shape, number_of, lean):
    loads = [min(1 << octave, number_of + 1 - (1 << octave)) * (1 << 20) // math.isqrt((1 << octave) ** lean) + 1 for octave in range((number_of + 1).bit_length()) if 1 << octave <= number_of]
    spread = 1 + sum(loads) // (1 << 30)
    grid = np.cumsum(np.array([max(1, weight // spread) for weight in loads]))
    ticket = jax.random.randint(jax.random.fold_in(own_key, 1), shape, 0, int(grid[len(loads) - 1]))
    start = jnp.left_shift(1, jnp.searchsorted(jnp.asarray(grid, jnp.int32), ticket, side="right").astype(jnp.int32))
    standing = start - 1 + jax.random.randint(jax.random.fold_in(own_key, 4), shape, 0, 1 << 30) % jnp.minimum(start, number_of + 1 - start)
    return jax.random.permutation(jax.random.fold_in(own_key, 2), number_of)[standing].astype(jnp.int32)


def setup_inputs(seed: int = 0) -> dict:
    splits = jax.random.split(jax.random.key(seed), 6)
    return {
        "hidden": draw_hidden(jax.random.fold_in(splits[5], 71), 0),
        "norm_gain": jnp.clip(1.0 + 0.1 * jax.random.normal(splits[1], (D,), jnp.float32), 0.5, 1.5),
        "weight": draw_weight(jax.random.fold_in(splits[5], 71), 0),
        "targets": set_ends(wide_ids(splits[3], (TOKENS,), VOCAB, 2), jax.random.fold_in(splits[3], 3), 0, VOCAB - 1).astype(jnp.int32),
        "label_mask": draw_label_mask(jax.random.fold_in(splits[5], 71), 0),
    }


epsilon = 1e-06

def normalize(hidden, norm_gain):
    values = hidden.astype(jnp.float32)
    squares = lax.optimization_barrier(jnp.mean(values * values, axis=-1, keepdims=True))
    return (values * lax.rsqrt(squares + epsilon) * norm_gain).astype(jnp.bfloat16)

def block_stats(row_block, label_block, weight_block, column_base):
    logits = jnp.dot(row_block, weight_block, preferred_element_type=jnp.float32)
    top_value = lax.optimization_barrier(jnp.max(logits, axis=1))
    exp_total = lax.optimization_barrier(jnp.sum(jnp.exp(logits - top_value[:, None]), axis=1))
    columns = column_base + lax.broadcasted_iota(jnp.int32, (1, logits.shape[1]), 1)
    target_logit = lax.optimization_barrier(jnp.sum(jnp.where(columns == label_block[:, None], logits, jnp.zeros_like(logits)), axis=1))
    return (top_value, exp_total, target_logit)

def combine_stats(first, second):
    top_value = jnp.maximum(first[0], second[0])
    exp_total = first[1] * jnp.exp(first[0] - top_value) + second[1] * jnp.exp(second[0] - top_value)
    return (top_value, exp_total, first[2] + second[2])

def reference(hidden, norm_gain, weight, targets, label_mask):
    normed = normalize(hidden, norm_gain)
    labels = jnp.where(label_mask == 1, targets, -1).astype(jnp.int32)
    counted = jnp.sum(label_mask, dtype=jnp.int32)
    block_width = VOC_DEV * N_VOC

    def vocab_step(block_index, running):
        first_column = (block_index * block_width).astype(jnp.int32)
        weight_block = lax.dynamic_slice_in_dim(weight, first_column, block_width, 1)
        return combine_stats(running, block_stats(normed, labels, weight_block, first_column))
    rows = normed.shape[0]
    initial = (jnp.full((rows,), -jnp.inf, jnp.float32), jnp.zeros((rows,), jnp.float32), jnp.zeros((rows,), jnp.float32))
    top_value, exp_total, target_logit = lax.fori_loop(0, N_TOK, vocab_step, initial)
    log_total = top_value + jnp.log(exp_total)
    per_token = label_mask.astype(jnp.float32) * (log_total - target_logit)
    counted_float = counted.astype(jnp.float32)
    token_loss = per_token * TOKENS / counted_float
    mean_loss = jnp.sum(per_token) / counted_float
    return (token_loss, mean_loss)
```

```python
import jax
import jax.numpy as jnp
from jax import lax
from jax.sharding import Mesh
from jax.sharding import PartitionSpec as P


Z, Y, C, X = 8, 4, 2, 4
ALL = ("z", "y", "c", "x")
EXTRA = 128
DIGIT = 64
epsilon = 1e-06


def pairs(move):
    out = []
    for z in range(Z):
        for y in range(Y):
            for c in range(C):
                for x in range(X):
                    tz, ty, tc, tx = move(z, y, c, x)
                    source = ((z * Y + y) * C + c) * X + x
                    target = (((tz % Z) * Y + ty % Y) * C + tc % C) * X + tx % X
                    out.append((source, target))
    return out


def send(value, move):
    return lax.ppermute(value, ALL, pairs(move))


def along_z(k):
    return lambda z, y, c, x: (z + k, y, c, x)


def along_mid(k):
    return lambda z, y, c, x: (z, y + k, c, x) if c == 0 else (z, y, c, x + k)


def along_last(k):
    return lambda z, y, c, x: (z, y, c, x + k) if c == 0 else (z, y + k, c, x)


def other_core(z, y, c, x):
    return (z, y, 1 - c, x)


def put(buffer, value, place):
    return lax.dynamic_update_slice_in_dim(buffer, value[None], place, 0)


def normalize(hidden, norm_gain):
    values = hidden.astype(jnp.float32)
    squares = jnp.mean(values * values, axis=-1, keepdims=True)
    return (values * lax.rsqrt(squares + epsilon) * norm_gain).astype(jnp.bfloat16)


def with_labels(normed, labels):
    code = (labels + 1)[:, None]
    lane = lax.broadcasted_iota(jnp.int32, (labels.shape[0], EXTRA), 1)
    digit = jnp.where(lane == 0, code % DIGIT, 0)
    digit = jnp.where(lane == 1, (code // DIGIT) % DIGIT, digit)
    digit = jnp.where(lane == 2, code // (DIGIT * DIGIT), digit)
    return jnp.concatenate([normed, digit.astype(jnp.bfloat16)], axis=1)


def labels_of(rows, width):
    digit = rows[:, width : width + 3].astype(jnp.float32)
    code = digit[:, 0] + DIGIT * digit[:, 1] + (DIGIT * DIGIT) * digit[:, 2]
    return code.astype(jnp.int32) - 1


def block_stats(rows, labels, weight, column_base):
    logits = jnp.dot(rows, weight, preferred_element_type=jnp.float32)
    top = jnp.max(logits, axis=1)
    total = jnp.sum(jnp.exp(logits - top[:, None]), axis=1)
    columns = column_base + lax.broadcasted_iota(jnp.int32, (1, logits.shape[1]), 1)
    target = jnp.sum(jnp.where(columns == labels[:, None], logits, 0.0), axis=1)
    return top + jnp.log(total), target


def chunk_stats(chunk, weights, bases, width):
    labels = labels_of(chunk, width)
    rows = chunk[:, :width]
    parts = [block_stats(rows, labels, w, b) for w, b in zip(weights, bases)]
    log_total = jnp.logaddexp(parts[0][0], parts[1][0])
    return jnp.stack([log_total, parts[0][1] + parts[1][1]]), (labels >= 0)


def merged(stats, axis):
    top = jnp.max(stats[:, 0], axis=0)
    total = jnp.sum(jnp.exp(stats[:, 0] - top), axis=0)
    return jnp.stack([top + jnp.log(total), jnp.sum(stats[:, 1], axis=0)])


def everyone(value, axes, count):
    copies = jnp.broadcast_to(value.reshape(1, -1), (count, value.size))
    return lax.all_to_all(copies, axes, 0, 0, tiled=True).reshape(count, *value.shape)


def body(hidden, norm_gain, weight, targets, label_mask):
    width = hidden.shape[1]
    local = hidden.shape[0]
    vocab = weight.shape[1]
    z, y, c, x = (lax.axis_index(a) for a in ALL)
    mid = jnp.where(c == 0, y, x)
    last = jnp.where(c == 0, x, y)
    other_weight = send(weight, other_core)
    own_base = (((z * Y + y) * C + c) * X + x) * vocab
    other_base = (((z * Y + y) * C + 1 - c) * X + x) * vocab

    labels = jnp.where(label_mask == 1, targets, -1)
    block = with_labels(normalize(hidden, norm_gain), labels)

    up1, down1 = send(block, along_z(1)), send(block, along_z(-1))
    up2, down2 = send(block, along_z(2)), send(block, along_z(-2))
    far = send(jnp.stack([up1, up2]), along_z(2))
    down3 = send(down1, along_z(-2))
    ring = jnp.zeros((Z, *block.shape), block.dtype)
    for k, value in ((0, block), (-1, up1), (1, down1), (-2, up2), (2, down2), (-3, far[0]), (-4, far[1]), (3, down3)):
        ring = put(ring, value, (z + k) % Z)

    chunk = ring.reshape(Z * local, -1)
    half = Z * local // 2
    up1, down1 = send(chunk, along_mid(1)), send(chunk, along_mid(-1))
    up2, down2 = send(up1[:half], along_mid(1)), send(down1[half:], along_mid(-1))
    plane = jnp.zeros((4, *chunk.shape), chunk.dtype)
    for k, value in ((0, chunk), (-1, up1), (1, down1), (2, jnp.concatenate([up2, down2]))):
        plane = put(plane, value, (mid + k) % 4)

    chunk = plane.reshape(4 * Z * local, -1)
    half = chunk.shape[0] // 2
    up1, down1 = send(chunk, along_last(1)), send(chunk, along_last(-1))
    up2, down2 = send(up1[:half], along_last(1)), send(down1[half:], along_last(-1))
    weights, bases = (weight, other_weight), (own_base, other_base)
    own = chunk_stats(chunk, weights, bases, width)
    before = chunk_stats(up1, weights, bases, width)
    after = chunk_stats(down1, weights, bases, width)
    across = chunk_stats(jnp.concatenate([up2, down2]), weights, bases, width)
    relative = jnp.stack([own[0], after[0], across[0], before[0]])
    valid = jnp.stack([own[1], after[1], across[1], before[1]])
    stats = jnp.roll(relative, last, axis=0)
    valid = jnp.roll(valid, last, axis=0).reshape(-1)

    stats = stats.transpose(1, 0, 2).reshape(2, -1)
    stats = merged(everyone(stats, ("y", "x"), Y * X), 0)
    stats = merged(everyone(stats, ("z",), Z), 0)

    per_token = jnp.where(valid, stats[0] - stats[1], 0.0)
    sums = jnp.stack([jnp.sum(per_token), jnp.sum(valid.astype(jnp.float32))])
    sums = sums + send(sums, other_core)
    start = ((last * 4 + mid) * Z + z) * local
    own_tokens = lax.dynamic_slice_in_dim(per_token, start, local, 0)
    everything = local * Z * Y * C * X
    token_loss = own_tokens * everything / sums[1]
    return token_loss, sums[0] / sums[1]


def solution(mesh):
    finer = Mesh(mesh.devices.reshape(Z, Y, C, X), ALL)
    in_specs = (P(ALL, None), P(), P(None, ALL), P(ALL), P(ALL))
    out_specs = (P(ALL), P())
    return jax.shard_map(body, mesh=finer, in_specs=in_specs, out_specs=out_specs, check_vma=False)
```

```python
import functools

import jax
import jax.numpy as jnp
from jax import lax
from jax.experimental import pallas as pl
from jax.experimental.pallas import tpu as pltpu
from jax.sharding import Mesh
from jax.sharding import PartitionSpec as P


Z, Y, C, X = 8, 4, 2, 4
ALL = ("z", "y", "c", "x")
ROWS = 8
WIDTH = 3584
EXTRA = 128
VOCAB = 594
HALF = 16 * ROWS
CUTS = 4
INVALID = -1e30
epsilon = 1e-06


def pairs(move):
    out = []
    for z in range(Z):
        for y in range(Y):
            for c in range(C):
                for x in range(X):
                    tz, ty, tc, tx = move(z, y, c, x)
                    source = ((z * Y + y) * C + c) * X + x
                    target = (((tz % Z) * Y + ty % Y) * C + tc % C) * X + tx % X
                    out.append((source, target))
    return out


def send(value, move):
    return lax.ppermute(value, ALL, pairs(move))


def along_z(k):
    return lambda z, y, c, x: (z + k, y, c, x)


def along_mid(k):
    return lambda z, y, c, x: (z, y + k, c, x) if c == 0 else (z, y, c, x + k)


def along_last(k):
    return lambda z, y, c, x: (z, y, c, x + k) if c == 0 else (z, y + k, c, x)


def other_core(z, y, c, x):
    return (z, y, 1 - c, x)


def place():
    z, y, c, x = (lax.axis_index(a) for a in ALL)
    mid = jnp.where(c == 0, y, x)
    last = jnp.where(c == 0, x, y)
    own = ((z * Y + y) * C + c) * X + x
    other = ((z * Y + y) * C + 1 - c) * X + x
    return z, c, mid, last, own, other


def normalize_kernel(hidden_ref, gain_ref, targets_ref, mask_ref, out_ref):
    values = hidden_ref[...].astype(jnp.float32)
    squares = jnp.mean(values * values, axis=-1, keepdims=True)
    normed = values * lax.rsqrt(squares + epsilon) * gain_ref[...]
    out_ref[:, :WIDTH] = normed.astype(jnp.bfloat16)
    row = lax.broadcasted_iota(jnp.int32, (ROWS, EXTRA), 0)
    lane = lax.broadcasted_iota(jnp.int32, (ROWS, EXTRA), 1)
    code = jnp.zeros((ROWS, EXTRA), jnp.int32)
    for i in range(ROWS):
        code = jnp.where(row == i, jnp.where(mask_ref[i] == 1, targets_ref[i] + 1, 0), code)
    digit = jnp.where(lane == 0, code & 63, 0)
    digit = jnp.where(lane == 1, (code >> 6) & 63, digit)
    digit = jnp.where(lane == 2, code >> 12, digit)
    out_ref[:, WIDTH:] = digit.astype(jnp.float32).astype(jnp.bfloat16)


def normalize(hidden, norm_gain, targets, label_mask):
    vmem, smem = pl.BlockSpec(memory_space=pltpu.VMEM), pl.BlockSpec(memory_space=pltpu.SMEM)
    return pl.pallas_call(
        normalize_kernel,
        out_shape=jax.ShapeDtypeStruct((ROWS, WIDTH + EXTRA), jnp.bfloat16),
        in_specs=[vmem, vmem, smem, smem],
        out_specs=vmem,
        name="normalize",
    )(hidden, norm_gain.reshape(1, WIDTH), targets, label_mask)


NT = (((1,), (1,)), ((), ()))


def chunk_kernel(chunks, final, *refs):
    n_half = 2 * chunks
    halves, weights = refs[:n_half], refs[n_half : n_half + 2]
    rest = refs[n_half + 2 :]
    if final:
        own_ref, sides_ref, out_ref, rows_ref, *weight_refs, logits_ref, all_ref, sems = rest
    else:
        out_ref, rows_ref, *weight_refs, logits_ref, sems = rest
    _, _, mid, last, own, other = place()
    count = chunks * 2 * HALF
    step = WIDTH // CUTS
    row_copies, weight_copies = [], []
    for k in range(CUTS):
        cut = pl.ds(k * step, step if k < CUTS - 1 else step + EXTRA)
        row_copies.append(
            [
                pltpu.make_async_copy(halves[h].at[:, cut], rows_ref.at[pl.ds(h * HALF, HALF), cut], sems.at[h, k])
                for h in range(n_half)
            ]
        )
        cut = pl.ds(k * step, step)
        weight_copies.append(
            [
                pltpu.make_async_copy(weights[w].at[:, cut], weight_refs[w].at[:, cut], sems.at[n_half + w, k])
                for w in range(2)
            ]
        )
    for k in range(CUTS):
        weight_copies[k][0].start()
        for copy in row_copies[k]:
            copy.start()
    for k in range(CUTS):
        weight_copies[k][1].start()

    labels = None
    parts = []
    for w in range(2):
        for k in range(CUTS):
            if w == 0:
                for copy in row_copies[k]:
                    copy.wait()
            weight_copies[k][w].wait()
            cut = slice(k * step, (k + 1) * step)
            product = lax.dot_general(
                weight_refs[w][:, cut], rows_ref[:, cut], NT, preferred_element_type=jnp.float32
            )
            if k == 0:
                logits_ref[...] = product
            else:
                logits_ref[...] += product
        if labels is None:
            lane = lax.broadcasted_iota(jnp.int32, (8, EXTRA), 1)
            power = jnp.where(lane == 0, 1, jnp.where(lane == 1, 64, jnp.where(lane == 2, 4096, 0)))
            code = lax.dot_general(
                power.astype(jnp.float32).astype(jnp.bfloat16), rows_ref[:, WIDTH:], NT, preferred_element_type=jnp.float32
            )
            labels = code[:1].astype(jnp.int32) - 1
        logits = logits_ref[...]
        top = jnp.max(logits, axis=0, keepdims=True)
        total = jnp.sum(jnp.exp(logits - top), axis=0, keepdims=True)
        column = lax.broadcasted_iota(jnp.int32, logits.shape, 0) + (own, other)[w] * VOCAB
        target = jnp.sum(jnp.where(column == labels, logits, 0.0), axis=0, keepdims=True)
        parts.append((top, total, target))
    top = jnp.maximum(parts[0][0], parts[1][0])
    total = parts[0][1] * jnp.exp(parts[0][0] - top) + parts[1][1] * jnp.exp(parts[1][0] - top)
    log_total = jnp.where(labels >= 0, top + jnp.log(total), INVALID)
    target = parts[0][2] + parts[1][2]
    both = jnp.concatenate([log_total, target, jnp.zeros((6, count), jnp.float32)], axis=0)
    found = []
    for i in range(chunks):
        turned = pltpu.roll(both[:, i * 256 : (i + 1) * 256], mid * 64, 1)
        found.append(turned)
    if not final:
        for i, turned in enumerate(found):
            out_ref[4 * i : 4 * i + 2] = turned[:2, :128]
            out_ref[4 * i + 2 : 4 * i + 4] = turned[:2, 128:]
        return
    chunk_rows = {
        0: (own_ref[0:1], own_ref[2:3], own_ref[1:2], own_ref[3:4]),
        1: (sides_ref[0:1], sides_ref[2:3], sides_ref[1:2], sides_ref[3:4]),
        2: (found[0][0:1, :128], found[0][0:1, 128:], found[0][1:2, :128], found[0][1:2, 128:]),
        3: (sides_ref[4:5], sides_ref[6:7], sides_ref[5:6], sides_ref[7:8]),
    }
    for k, (first, second, first_target, second_target) in chunk_rows.items():
        at = 2 * ((last + k) % 4)
        all_ref[pl.ds(at, 1)] = first
        all_ref[pl.ds(at + 1, 1)] = second
        all_ref[pl.ds(at + 8, 1)] = first_target
        all_ref[pl.ds(at + 9, 1)] = second_target
    everything = all_ref[...]
    for i in range(Z):
        out_ref[i] = everything


def chunk_stats(halves, weights, before=None):
    chunks = len(halves) // 2
    final = before is not None
    count = chunks * 2 * HALF
    anywhere, vmem = pl.BlockSpec(memory_space=pl.ANY), pl.BlockSpec(memory_space=pltpu.VMEM)
    shape = (Z, 16, 128) if final else (4 * chunks, 128)
    scratch = [
        pltpu.VMEM((count, WIDTH + EXTRA), jnp.bfloat16),
        pltpu.VMEM((VOCAB, WIDTH), jnp.bfloat16),
        pltpu.VMEM((VOCAB, WIDTH), jnp.bfloat16),
        pltpu.VMEM((VOCAB, count), jnp.float32),
    ]
    if final:
        scratch.append(pltpu.VMEM((16, 128), jnp.float32))
    scratch.append(pltpu.SemaphoreType.DMA((2 * chunks + 2, CUTS)))
    return pl.pallas_call(
        functools.partial(chunk_kernel, chunks, final),
        out_shape=jax.ShapeDtypeStruct(shape, jnp.float32),
        in_specs=[anywhere] * (2 * chunks + 2) + [vmem] * (2 if final else 0),
        out_specs=vmem,
        scratch_shapes=scratch,
        compiler_params=pltpu.CompilerParams(vmem_limit_bytes=40 * 2**20),
        cost_estimate=pl.CostEstimate(
            flops=2 * count * 2 * VOCAB * WIDTH,
            bytes_accessed=4 * VOCAB * WIDTH + 2 * count * WIDTH,
            transcendentals=count * 2 * VOCAB,
        ),
        name=f"chunk_stats_{chunks}_{final}",
    )(*halves, *weights, *(before or ()))


def merge(rows):
    top = functools.reduce(jnp.maximum, [r[0] for r in rows])
    total = sum(jnp.exp(r[0] - top) for r in rows)
    return top, total, sum(r[1] for r in rows)


def merge_z_kernel(in_ref, out_ref):
    rows = [(in_ref[i, :8], in_ref[i, 8:]) for i in range(Z)]
    top, total, target = merge(rows)
    log_total = top + jnp.log(total)
    for i in range(Y * C * X):
        out_ref[i, :8] = log_total
        out_ref[i, 8:] = target


def loss_kernel(in_ref, tokens_ref, mean_ref):
    z, core, mid, last, _, _ = place()
    loss_sum, counted, own = 0.0, 0.0, None
    for c in range(C):
        rows = []
        for y in range(Y):
            for x in range(X):
                i = (y * C + c) * X + x
                rows.append((in_ref[i, :8], in_ref[i, 8:]))
        top, total, target = merge(rows)
        valid = top > 0.5 * INVALID
        loss = jnp.where(valid, top + jnp.log(total) - target, 0.0)
        loss_sum += jnp.sum(loss)
        counted += jnp.sum(valid.astype(jnp.float32))
        own = loss if own is None else jnp.where(core == c, loss, own)
    scaled = own * (ROWS * Z * Y * C * X) / jnp.full(own.shape, counted)
    start = ((last * 4 + mid) * Z + z) * ROWS
    index = lax.broadcasted_iota(jnp.int32, own.shape, 0) * 128 + lax.broadcasted_iota(jnp.int32, own.shape, 1)
    for i in range(ROWS):
        tokens_ref[i] = jnp.sum(jnp.where(index == start + i, scaled, 0.0))
    mean = jnp.full((8, 128), loss_sum) / jnp.full((8, 128), counted)
    mean_ref[0] = jnp.max(mean)


def small_call(kernel, value, out_shape, out_specs, name):
    return pl.pallas_call(
        kernel,
        out_shape=out_shape,
        in_specs=[pl.BlockSpec(memory_space=pltpu.VMEM)],
        out_specs=out_specs,
        name=name,
    )(value)


def body(hidden, norm_gain, weight, targets, label_mask):
    z = lax.axis_index("z")
    own_weight = weight.T
    other_weight = send(own_weight, other_core)
    block = normalize(hidden, norm_gain, targets, label_mask)

    up1, down1 = send(block, along_z(1)), send(block, along_z(-1))
    up2, down2 = send(block, along_z(2)), send(block, along_z(-2))
    far = send(jnp.stack([up1, up2]), along_z(2))
    down3 = send(down1, along_z(-2))
    ring = jnp.zeros((Z, *block.shape), block.dtype)
    for k, value in ((0, block), (-1, up1), (1, down1), (-2, up2), (2, down2), (-3, far[0]), (-4, far[1]), (3, down3)):
        ring = lax.dynamic_update_slice_in_dim(ring, value[None], (z + k) % Z, 0)

    chunk = ring.reshape(Z * ROWS, -1)
    half = Z * ROWS // 2
    up1, down1 = send(chunk, along_mid(1)), send(chunk, along_mid(-1))
    up2, down2 = send(chunk[:half], along_mid(2)), send(chunk[half:], along_mid(-2))
    first = jnp.concatenate([chunk, down1])
    second = jnp.concatenate([up2, down2, up1])

    up_first, down_first = send(first, along_last(1)), send(first, along_last(-1))
    down_second, up_second = send(second, along_last(-1)), send(second, along_last(1))
    up_up, down_down = send(up_first, along_last(1)), send(down_second, along_last(-1))
    other_weight, first, second = lax.optimization_barrier((other_weight, first, second))
    weights = (own_weight, other_weight)
    own = chunk_stats((first, second), weights)
    sides = chunk_stats((down_first, down_second, up_first, up_second), weights)
    copies = chunk_stats((up_up, down_down), weights, (own, sides))

    vmem, smem = pl.BlockSpec(memory_space=pltpu.VMEM), pl.BlockSpec(memory_space=pltpu.SMEM)
    stats = lax.all_to_all(copies, "z", 0, 0, tiled=True)
    shape = jax.ShapeDtypeStruct((Y * C * X, 16, 128), jnp.float32)
    copies = small_call(merge_z_kernel, stats, shape, vmem, "merge_z")
    stats = lax.all_to_all(copies, ("y", "c", "x"), 0, 0, tiled=True)
    shapes = (jax.ShapeDtypeStruct((ROWS,), jnp.float32), jax.ShapeDtypeStruct((1,), jnp.float32))
    token_loss, mean_loss = small_call(loss_kernel, stats, shapes, (smem, smem), "loss")
    return token_loss, mean_loss.reshape(())


def solution(mesh):
    finer = Mesh(mesh.devices.reshape(Z, Y, C, X), ALL)
    in_specs = (P(ALL, None), P(), P(None, ALL), P(ALL), P(ALL))
    out_specs = (P(ALL), P())
    return jax.shard_map(body, mesh=finer, in_specs=in_specs, out_specs=out_specs, check_vma=False)
```

```python
import functools

import jax
import jax.numpy as jnp
from jax import lax
from jax.experimental import pallas as pl
from jax.experimental.pallas import tpu as pltpu
from jax.sharding import Mesh
from jax.sharding import PartitionSpec as P


Z, Y, C, X = 8, 4, 2, 4
ALL = ("z", "y", "c", "x")
ROWS = 8
WIDTH = 3584
EXTRA = 128
VOCAB = 594
HALF = 16 * ROWS
CUTS = 4
INVALID = -1e30
epsilon = 1e-06


def pairs(move):
    out = []
    for z in range(Z):
        for y in range(Y):
            for c in range(C):
                for x in range(X):
                    tz, ty, tc, tx = move(z, y, c, x)
                    source = ((z * Y + y) * C + c) * X + x
                    target = (((tz % Z) * Y + ty % Y) * C + tc % C) * X + tx % X
                    out.append((source, target))
    return out


def send(value, move):
    return lax.ppermute(value, ALL, pairs(move))


def along_z(k):
    return lambda z, y, c, x: (z + k, y, c, x)


def along_mid(k):
    return lambda z, y, c, x: (z, y + k, c, x) if c == 0 else (z, y, c, x + k)


def along_last(k):
    return lambda z, y, c, x: (z, y, c, x + k) if c == 0 else (z, y + k, c, x)


def other_core(z, y, c, x):
    return (z, y, 1 - c, x)


def place():
    z, y, c, x = (lax.axis_index(a) for a in ALL)
    mid = jnp.where(c == 0, y, x)
    last = jnp.where(c == 0, x, y)
    own = ((z * Y + y) * C + c) * X + x
    other = ((z * Y + y) * C + 1 - c) * X + x
    return z, c, mid, last, own, other


def normalize_kernel(hidden_ref, gain_ref, targets_ref, mask_ref, out_ref):
    values = hidden_ref[...].astype(jnp.float32)
    squares = jnp.mean(values * values, axis=-1, keepdims=True)
    normed = values * lax.rsqrt(squares + epsilon) * gain_ref[...][None, :]
    out_ref[:, :WIDTH] = normed.astype(jnp.bfloat16)
    row = lax.broadcasted_iota(jnp.int32, (ROWS, EXTRA), 0)
    lane = lax.broadcasted_iota(jnp.int32, (ROWS, EXTRA), 1)
    code = jnp.zeros((ROWS, EXTRA), jnp.int32)
    for i in range(ROWS):
        code = jnp.where(row == i, jnp.where(mask_ref[i] == 1, targets_ref[i] + 1, 0), code)
    digit = jnp.where(lane == 0, code & 63, 0)
    digit = jnp.where(lane == 1, (code >> 6) & 63, digit)
    digit = jnp.where(lane == 2, code >> 12, digit)
    out_ref[:, WIDTH:] = digit.astype(jnp.float32).astype(jnp.bfloat16)


def normalize(hidden, norm_gain, targets, label_mask):
    vmem, smem = pl.BlockSpec(memory_space=pltpu.VMEM), pl.BlockSpec(memory_space=pltpu.SMEM)
    return pl.pallas_call(
        normalize_kernel,
        out_shape=jax.ShapeDtypeStruct((ROWS, WIDTH + EXTRA), jnp.bfloat16),
        in_specs=[vmem, vmem, smem, smem],
        out_specs=vmem,
        name="normalize",
    )(hidden, norm_gain, targets, label_mask)


NT = (((1,), (1,)), ((), ()))


def chunk_kernel(chunks, final, *refs):
    n_half = 2 * chunks
    halves, weight_refs = refs[:n_half], refs[n_half : n_half + 2]
    rest = refs[n_half + 2 :]
    if final:
        own_ref, sides_ref, out_ref, rows_ref, logits_ref, all_ref, sems = rest
    else:
        out_ref, rows_ref, logits_ref, sems = rest
    _, _, mid, last, own, other = place()
    count = chunks * 2 * HALF
    step = WIDTH // CUTS
    row_copies = []
    for k in range(CUTS):
        cut = pl.ds(k * step, step if k < CUTS - 1 else step + EXTRA)
        row_copies.append(
            [
                pltpu.make_async_copy(halves[h].at[:, cut], rows_ref.at[pl.ds(h * HALF, HALF), cut], sems.at[h, k])
                for h in range(n_half)
            ]
        )
    for k in range(CUTS):
        for copy in row_copies[k]:
            copy.start()

    labels = None
    parts = []
    for w in range(2):
        for k in range(CUTS):
            if w == 0:
                for copy in row_copies[k]:
                    copy.wait()
            cut = slice(k * step, (k + 1) * step)
            product = lax.dot_general(
                weight_refs[w][:, cut], rows_ref[:, cut], NT, preferred_element_type=jnp.float32
            )
            if k == 0:
                logits_ref[...] = product
            else:
                logits_ref[...] += product
        if labels is None:
            lane = lax.broadcasted_iota(jnp.int32, (8, EXTRA), 1)
            power = jnp.where(lane == 0, 1, jnp.where(lane == 1, 64, jnp.where(lane == 2, 4096, 0)))
            code = lax.dot_general(
                power.astype(jnp.float32).astype(jnp.bfloat16), rows_ref[:, WIDTH:], NT, preferred_element_type=jnp.float32
            )
            labels = code[:1].astype(jnp.int32) - 1
        logits = logits_ref[...]
        top = jnp.max(logits, axis=0, keepdims=True)
        total = jnp.sum(jnp.exp(logits - top), axis=0, keepdims=True)
        column = lax.broadcasted_iota(jnp.int32, logits.shape, 0) + (own, other)[w] * VOCAB
        target = jnp.sum(jnp.where(column == labels, logits, 0.0), axis=0, keepdims=True)
        parts.append((top, total, target))
    top = jnp.maximum(parts[0][0], parts[1][0])
    total = parts[0][1] * jnp.exp(parts[0][0] - top) + parts[1][1] * jnp.exp(parts[1][0] - top)
    log_total = jnp.where(labels >= 0, top + jnp.log(total), INVALID)
    target = parts[0][2] + parts[1][2]
    both = jnp.concatenate([log_total, target, jnp.zeros((6, count), jnp.float32)], axis=0)
    found = []
    for i in range(chunks):
        turned = pltpu.roll(both[:, i * 256 : (i + 1) * 256], mid * 64, 1)
        found.append(turned)
    if not final:
        for i, turned in enumerate(found):
            out_ref[4 * i : 4 * i + 2] = turned[:2, :128]
            out_ref[4 * i + 2 : 4 * i + 4] = turned[:2, 128:]
        return
    chunk_rows = {
        0: (own_ref[0:1], own_ref[2:3], own_ref[1:2], own_ref[3:4]),
        1: (sides_ref[0:1], sides_ref[2:3], sides_ref[1:2], sides_ref[3:4]),
        2: (found[0][0:1, :128], found[0][0:1, 128:], found[0][1:2, :128], found[0][1:2, 128:]),
        3: (sides_ref[4:5], sides_ref[6:7], sides_ref[5:6], sides_ref[7:8]),
    }
    for k, (first, second, first_target, second_target) in chunk_rows.items():
        at = 2 * ((last + k) % 4)
        all_ref[pl.ds(at, 1)] = first
        all_ref[pl.ds(at + 1, 1)] = second
        all_ref[pl.ds(at + 8, 1)] = first_target
        all_ref[pl.ds(at + 9, 1)] = second_target
    everything = all_ref[...]
    for i in range(Y * X):
        out_ref[i] = everything


def chunk_stats(halves, weights, before=None):
    chunks = len(halves) // 2
    final = before is not None
    count = chunks * 2 * HALF
    anywhere, vmem = pl.BlockSpec(memory_space=pl.ANY), pl.BlockSpec(memory_space=pltpu.VMEM)
    shape = (Y * X, 16, 128) if final else (4 * chunks, 128)
    scratch = [
        pltpu.VMEM((count, WIDTH + EXTRA), jnp.bfloat16),
        pltpu.VMEM((VOCAB, count), jnp.float32),
    ]
    if final:
        scratch.append(pltpu.VMEM((16, 128), jnp.float32))
    scratch.append(pltpu.SemaphoreType.DMA((2 * chunks, CUTS)))
    return pl.pallas_call(
        functools.partial(chunk_kernel, chunks, final),
        out_shape=jax.ShapeDtypeStruct(shape, jnp.float32),
        in_specs=[anywhere] * (2 * chunks) + [vmem] * (4 if final else 2),
        out_specs=vmem,
        scratch_shapes=scratch,
        compiler_params=pltpu.CompilerParams(vmem_limit_bytes=40 * 2**20),
        cost_estimate=pl.CostEstimate(
            flops=2 * count * 2 * VOCAB * WIDTH,
            bytes_accessed=4 * VOCAB * WIDTH + 2 * count * WIDTH,
            transcendentals=count * 2 * VOCAB,
        ),
        name=f"chunk_stats_{chunks}_{final}",
    )(*halves, *weights, *(before or ()))


def merge(rows):
    top = functools.reduce(jnp.maximum, [r[0] for r in rows])
    total = sum(jnp.exp(r[0] - top) for r in rows)
    return top, total, sum(r[1] for r in rows)


def merge_plane_kernel(in_ref, out_ref):
    rows = [(in_ref[i, :8], in_ref[i, 8:]) for i in range(Y * X)]
    top, total, target = merge(rows)
    log_total = top + jnp.log(total)
    for i in range(Z * C):
        out_ref[i, :8] = log_total
        out_ref[i, 8:] = target


def loss_kernel(in_ref, tokens_ref, mean_ref):
    z, core, mid, last, _, _ = place()
    loss_sum, counted, own = 0.0, 0.0, None
    for c in range(C):
        rows = []
        for i in range(c, Z * C, C):
            rows.append((in_ref[i, :8], in_ref[i, 8:]))
        top, total, target = merge(rows)
        valid = top > 0.5 * INVALID
        loss = jnp.where(valid, top + jnp.log(total) - target, 0.0)
        loss_sum += jnp.sum(loss)
        counted += jnp.sum(valid.astype(jnp.float32))
        own = loss if own is None else jnp.where(core == c, loss, own)
    scaled = own * (ROWS * Z * Y * C * X) / jnp.full(own.shape, counted)
    start = ((last * 4 + mid) * Z + z) * ROWS
    index = lax.broadcasted_iota(jnp.int32, own.shape, 0) * 128 + lax.broadcasted_iota(jnp.int32, own.shape, 1)
    for i in range(ROWS):
        tokens_ref[i] = jnp.sum(jnp.where(index == start + i, scaled, 0.0))
    mean = jnp.full((8, 128), loss_sum) / jnp.full((8, 128), counted)
    mean_ref[0] = jnp.max(mean)


def small_call(kernel, value, out_shape, out_specs, name):
    return pl.pallas_call(
        kernel,
        out_shape=out_shape,
        in_specs=[pl.BlockSpec(memory_space=pltpu.VMEM)],
        out_specs=out_specs,
        name=name,
    )(value)


def body(hidden, norm_gain, weight, targets, label_mask):
    z = lax.axis_index("z")
    own_weight = weight.T
    other_weight = send(own_weight, other_core)
    block = normalize(hidden, norm_gain, targets, label_mask)

    up1, down1 = send(block, along_z(1)), send(block, along_z(-1))
    up2, down2 = send(block, along_z(2)), send(block, along_z(-2))
    far = send(jnp.stack([up1, up2]), along_z(2))
    down3 = send(down1, along_z(-2))
    ring = jnp.zeros((Z, *block.shape), block.dtype)
    for k, value in ((0, block), (-1, up1), (1, down1), (-2, up2), (2, down2), (-3, far[0]), (-4, far[1]), (3, down3)):
        ring = lax.dynamic_update_slice_in_dim(ring, value[None], (z + k) % Z, 0)

    chunk = ring.reshape(Z * ROWS, -1)
    half = Z * ROWS // 2
    up1, down1 = send(chunk, along_mid(1)), send(chunk, along_mid(-1))
    up2, down2 = send(chunk[:half], along_mid(2)), send(chunk[half:], along_mid(-2))
    first = jnp.concatenate([chunk, down1])
    second = jnp.concatenate([up2, down2, up1])

    up_first, down_first = send(first, along_last(1)), send(first, along_last(-1))
    down_second, up_second = send(second, along_last(-1)), send(second, along_last(1))
    up_up, down_down = send(up_first, along_last(1)), send(down_second, along_last(-1))
    other_weight, first, second = lax.optimization_barrier((other_weight, first, second))
    weights = (own_weight, other_weight)
    own = chunk_stats((first, second), weights)
    sides = chunk_stats((down_first, down_second, up_first, up_second), weights)
    copies = chunk_stats((up_up, down_down), weights, (own, sides))

    vmem, smem = pl.BlockSpec(memory_space=pltpu.VMEM), pl.BlockSpec(memory_space=pltpu.SMEM)
    stats = lax.all_to_all(copies, ("y", "x"), 0, 0, tiled=True)
    shape = jax.ShapeDtypeStruct((Z * C, 16, 128), jnp.float32)
    copies = small_call(merge_plane_kernel, stats, shape, vmem, "merge_plane")
    stats = lax.all_to_all(copies, ("z", "c"), 0, 0, tiled=True)
    shapes = (jax.ShapeDtypeStruct((ROWS,), jnp.float32), jax.ShapeDtypeStruct((1,), jnp.float32))
    token_loss, mean_loss = small_call(loss_kernel, stats, shapes, (smem, smem), "loss")
    return token_loss, mean_loss.reshape(())


def solution(mesh):
    finer = Mesh(mesh.devices.reshape(Z, Y, C, X), ALL)
    in_specs = (P(ALL, None), P(), P(None, ALL), P(ALL), P(ALL))
    out_specs = (P(ALL), P())
    return jax.shard_map(body, mesh=finer, in_specs=in_specs, out_specs=out_specs, check_vma=False)
```
